32 devices in a mesh: tm: 4 (over y, core), lev: 8 (over z, x).
Axes of the slice: x: 2, y: 2, z: 4, core: 2. Of those that a mesh axis runs over, the one named last changes fastest.
Arguments:
- obs_cell: int32 [4, 16384], P('tm'), may hold values from 0 to 65535
- innovation: float32 [4, 64, 16384], P('tm', 'lev'), may hold values from -8 to 8
- tangent: float32 [4, 64, 128, 512], P('tm', 'lev'), may hold values from -0.45 to 0.45
- damping: float32 [4, 64, 128], P('tm'), may hold values from 0.05 to 0.95
- spread: float32 [64, 128], replicated, may hold values from 0.5 to 2
- vertical: float32 [64, 64], replicated, may hold values from -0.75 to 0.75
Outputs:
- gradient: float32 [64, 128, 2, 128], P(None, 'lev', None, 'tm')
The draws below stay inside these ranges and needn't reach their ends.
All inputs are finite; a program needn't handle non-finite values.
Results may differ from the reference program's by a relative error of at most 0.0003.
Values sent between devices are 32-bit elements; how exact they have to be, the bound alone decides.
A program may use at most 128 MiB of HBM per device.

```python
import math
import jax
import jax.numpy as jnp
from jax import lax

NLAT = 128
NLON = 512
WAVES = 128
LEVELS = 64
OBS = 16384
TIMES = 4


def touch_ends(drawn, stream_key, smallest, top_value):
    index_at = [jax.random.randint(jax.random.fold_in(stream_key, axis), (), 0, length) for axis, length in enumerate(drawn.shape)]
    widest = drawn.shape.index(max(drawn.shape))
    next_to = index_at[:widest] + [(index_at[widest] + 1) % drawn.shape[widest]] + index_at[widest + 1:]
    return drawn.at[tuple(index_at)].set(smallest).at[tuple(next_to)].set(top_value)


def block_scale(own_key, dims, cuts, smallest, largest):
    gain = 1.0
    for position, shards_of in cuts:
        draws = jax.random.uniform(jax.random.fold_in(jax.random.fold_in(own_key, 6), position), (shards_of,), jnp.float32, smallest / len(cuts), largest / len(cuts))
        gain = gain * jnp.repeat(jnp.exp(draws), dims[position] // shards_of).reshape((-1,) + (1,) * (len(dims) - 1 - position))
    return gain


def bell_draw(key, shape, scale, most, shards=(), held_as=jnp.bfloat16):
    loudness = block_scale(key, shape, shards, -0.22, 0.18) if shards else 1.0
    entries = jax.random.normal(key, shape, jnp.float32) * scale * loudness
    return jnp.minimum(jnp.maximum(entries, -most), most).astype(held_as)


def setup_inputs(seed: int = 0) -> dict:
    key_of = jax.random.split(jax.random.key(seed), 7)
    obs_cell = touch_ends(jax.random.randint(key_of[0], (TIMES, OBS), 0, NLAT * NLON), jax.random.fold_in(key_of[0], 1), 0, (NLAT * NLON) - 1).astype(jnp.int32)
    innovation = bell_draw(key_of[1], (TIMES, LEVELS, OBS), 1.5, 8.0, ((0, 4), (1, 8)), jnp.float32)
    tangent = jnp.clip(jax.random.uniform(key_of[2], (TIMES, LEVELS, NLAT, NLON), jnp.float32, -0.45, 0.45) * block_scale(key_of[2], (TIMES, LEVELS, NLAT, NLON), ((0, 4), (1, 8)), -0.4, 0.0), -0.45, 0.45)
    damping = jnp.clip(jnp.exp(math.log(0.95) - 2.944439 * jax.random.uniform(key_of[3], (TIMES, LEVELS, WAVES), jnp.float32) ** block_scale(key_of[3], (TIMES, LEVELS, WAVES), ((0, 4),), -0.2, 0.2)), 0.05, 0.95)
    spread = jnp.clip(jnp.exp(jax.random.uniform(key_of[4], (LEVELS, WAVES), jnp.float32, math.log(0.5), math.log(2.0))), 0.5, 2.0)
    vertical = bell_draw(key_of[5], (LEVELS, LEVELS), LEVELS ** -0.5, 0.75, (), jnp.float32)
    return dict(obs_cell=obs_cell, innovation=innovation, tangent=tangent, damping=damping, spread=spread, vertical=vertical)


PRECISE = lax.Precision.HIGHEST
HALF_GAMMA_LOG = 0.5 * math.log(math.pi) - math.log(2.0)

def fourier_table(lon_count, wave_count):
    longitude = jnp.arange(lon_count, dtype=jnp.int32)[:, None]
    wavenumber = jnp.arange(wave_count, dtype=jnp.int32)[None, :]
    angles = (longitude * wavenumber % lon_count).astype(jnp.float32) * (2.0 * math.pi / lon_count)
    norm_factor = math.sqrt(2.0 / lon_count)
    columns = jnp.stack([jnp.cos(angles), jnp.sin(angles)], axis=2) * norm_factor
    return columns.reshape(lon_count, 2 * wave_count)

def legendre_table(first_wave, wave_block, lat_count, wave_count):
    orders = (first_wave + jnp.arange(wave_block, dtype=jnp.int32)).astype(jnp.float32)[:, None]
    row_index = jnp.arange(lat_count, dtype=jnp.float32)
    latitude = (row_index + 0.5) * (math.pi / lat_count) - 0.5 * math.pi
    sine_lat = jnp.sin(latitude)[None, :]
    cosine = jnp.cos(latitude)[None, :]
    logdiag = -0.5 * math.log(2.0) + 0.5 * (jax.scipy.special.gammaln(orders + 1.5) - HALF_GAMMA_LOG - jax.scipy.special.gammaln(orders + 1.0)) + orders * jnp.log(cosine)
    diagonal = jnp.exp(logdiag)

    def advance(state_pair, degree):
        prev_one, prev_two = state_pair
        upward = jnp.sqrt(jnp.maximum(4.0 * degree * degree - 1.0, 1.0) / jnp.maximum(degree * degree - orders * orders, 1.0))
        lower = degree - 1.0
        downward = jnp.sqrt(jnp.maximum(lower * lower - orders * orders, 0.0) / jnp.maximum(4.0 * lower * lower - 1.0, 1.0))
        recurred = upward * (sine_lat * prev_one - downward * prev_two)
        current = jnp.where(degree < orders, 0.0, jnp.where(degree == orders, diagonal, recurred))
        return ((current, prev_one), current)
    zero_rows = jnp.zeros((wave_block, lat_count), jnp.float32)
    degrees = jnp.arange(wave_count, dtype=jnp.float32)
    _, values = lax.scan(advance, (zero_rows, zero_rows), degrees, unroll=16)
    weight = jnp.sqrt(math.pi / lat_count * cosine)
    return values * weight[None]

def forcing_field(cell_ids, innov_rows, lat_count, lon_count):
    flat_field = jnp.zeros((innov_rows.shape[0], lat_count * lon_count), jnp.float32)
    flat_field = flat_field.at[:, cell_ids].add(innov_rows)
    return flat_field.reshape(innov_rows.shape[0], lat_count, lon_count)

def reference(obs_cell, innovation, tangent, damping, spread, vertical):
    fourier = fourier_table(NLON, WAVES)
    legendre = legendre_table(0, WAVES, NLAT, WAVES)
    adjoint = jnp.zeros((LEVELS, NLAT, NLON), jnp.float32)
    total = jnp.zeros((LEVELS, WAVES, 2, WAVES), jnp.float32)
    for time_step in range(TIMES - 1, -1, -1):
        forced = adjoint + forcing_field(obs_cell[time_step], innovation[time_step], NLAT, NLON)
        coeffs = jnp.einsum('klx,xc->klc', forced, fourier, precision=PRECISE)
        coeffs = coeffs.reshape(LEVELS, NLAT, WAVES, 2)
        spectral = jnp.einsum('klmp,nml->kmpn', coeffs, legendre, precision=PRECISE)
        total = total + spectral
        filtered = spectral * damping[time_step][:, None, None, :]
        synthesized = jnp.einsum('kmpn,nml->klmp', filtered, legendre, precision=PRECISE)
        synthesized = synthesized.reshape(LEVELS, NLAT, 2 * WAVES)
        adjoint = tangent[time_step] * forced + jnp.einsum('klc,xc->klx', synthesized, fourier, precision=PRECISE)
    scaled = total * spread[:, None, None, :]
    return jnp.einsum('kj,kmpn->jmpn', vertical, scaled, precision=PRECISE)
```

```python
import functools
import math

import jax
import jax.numpy as jnp
import numpy as np
from jax import lax
from jax.experimental import pallas as pl
from jax.experimental.pallas import tpu as pltpu
from jax.sharding import PartitionSpec as P

PRECISE = lax.Precision.HIGHEST
BF16 = jnp.bfloat16
F32 = jnp.float32
NT = (((1,), (1,)), ((), ()))
NN = (((1,), (0,)), ((), ()))
VMEM_BYTES = 62 * 1024 * 1024


def dot(left, right, dims):
    return lax.dot_general(left, right, dims, preferred_element_type=F32)


def halves(value):
    high = value.astype(BF16)
    return high, (value - high.astype(F32)).astype(BF16)


def fourier_rows(lon_count, wave_count):
    index = np.arange(wave_count)[:, None] * np.arange(lon_count)[None, :] % lon_count
    angles = 2.0 * np.pi * index / lon_count
    return (np.concatenate([np.cos(angles), np.sin(angles)], 0) * np.sqrt(2.0 / lon_count)).astype(np.float32)


def legendre_coefficients(lat_count, wave_count):
    phi = (np.arange(lat_count) + 0.5) * np.pi / lat_count - 0.5 * np.pi
    orders = np.arange(wave_count).astype(np.float64)
    lead = np.array(
        [
            -0.5 * math.log(2.0)
            + 0.5 * (math.lgamma(m + 1.5) - math.lgamma(1.5) - math.lgamma(m + 1.0))
            for m in range(wave_count)
        ]
    )
    weight = np.sqrt(np.pi * np.cos(phi) / lat_count)
    diagonal = weight[:, None] * np.exp(lead[None, :] + orders[None, :] * np.log(np.cos(phi))[:, None])
    mu = np.broadcast_to(np.sin(phi)[:, None], (lat_count, wave_count))
    degree = orders[:, None]
    above = degree > orders[None, :]
    gap = np.where(above, degree**2 - orders[None, :] ** 2, 1.0)
    up = np.where(above, np.sqrt(np.maximum(4.0 * degree**2 - 1.0, 0.0) / gap), 0.0)
    lower = degree - 1.0
    down = np.sqrt(np.maximum(lower**2 - orders[None, :] ** 2, 0.0) / np.maximum(4.0 * lower**2 - 1.0, 1.0))
    both = up * down
    return [np.asarray(a, np.float32) for a in (mu, diagonal, up, both)]


def forcing_kernel(lat_rows, lon_cols, cell_ref, innov_ref, out_ref):
    cells = cell_ref[0]
    width = cells.shape[1]
    rows = cells // lon_cols
    cols = cells - rows * lon_cols
    innov = innov_ref[0]
    levels = innov.shape[0]
    hit = lax.broadcasted_iota(jnp.int32, (lat_rows, width), 0) == rows
    spread_cols = jnp.where(
        lax.broadcasted_iota(jnp.int32, (lon_cols, width), 0) == cols, 1.0, 0.0
    ).astype(BF16)
    high = innov.astype(BF16).astype(F32)
    low = innov - high
    pieces = [jnp.where(hit, part[k : k + 1, :], 0.0).astype(BF16) for part in (high, low) for k in range(levels)]
    field = dot(jnp.concatenate(pieces, 0), spread_cols, NT)
    field = field[: levels * lat_rows] + field[levels * lat_rows :]

    @pl.when(pl.program_id(1) == 0)
    def _():
        out_ref[0] = field

    @pl.when(pl.program_id(1) > 0)
    def _():
        out_ref[0] += field


def forcing_fields(cells, innov, lat_rows, lon_cols):
    times, levels, count = innov.shape
    width = math.gcd(count, 2048)
    body = functools.partial(forcing_kernel, lat_rows, lon_cols)
    return pl.pallas_call(
        body,
        grid=(times, count // width),
        in_specs=[
            pl.BlockSpec((1, 1, width), lambda t, c: (t, 0, c)),
            pl.BlockSpec((1, levels, width), lambda t, c: (t, 0, c)),
        ],
        out_specs=pl.BlockSpec((1, levels * lat_rows, lon_cols), lambda t, c: (t, 0, 0)),
        out_shape=jax.ShapeDtypeStruct((times, levels * lat_rows, lon_cols), F32),
        compiler_params=pltpu.CompilerParams(vmem_limit_bytes=VMEM_BYTES),
        cost_estimate=pl.CostEstimate(
            flops=4 * times * levels * lat_rows * lon_cols * count, bytes_accessed=8 * 2**20, transcendentals=0
        ),
    )(cells.reshape(times, 1, count), innov)


def sweep_kernel(
    field_ref, tangent_ref, damp_ref, fhigh_ref, flow_ref, mu_ref, diag_ref, up_ref, both_ref,
    total_ref, table, high, low, packed, adjoint,
):
    times, rows, lon_cols = field_ref.shape
    lat_rows, waves = mu_ref.shape
    levels = rows // lat_rows
    group = damp_ref.shape[1]
    half = group // 2

    orders = lax.broadcasted_iota(jnp.int32, (lat_rows, waves), 1)

    def advance(n, state):
        one, two = state
        recurred = up_ref[pl.ds(n, 1), :] * (mu_ref[...] * one) - both_ref[pl.ds(n, 1), :] * two
        value = jnp.where(orders == n, diag_ref[...], recurred)
        table[pl.ds(n, waves, stride=waves), :] = value.T
        return value, one

    zero = 0.0 * mu_ref[...]
    lax.fori_loop(0, waves, advance, (zero, zero))

    def split(m, carry):
        upper, lower = halves(table[pl.ds(m * waves, waves), :])
        high[m] = upper
        low[m] = lower
        return carry

    lax.fori_loop(0, waves, split, 0, unroll=2)

    def pair_sum(value):
        return value + pltpu.roll(value, half, 0)

    in_high = lax.broadcasted_iota(jnp.int32, (group, waves), 0) < half
    adjoint[...] = jnp.zeros_like(adjoint)
    total_ref[...] = jnp.zeros_like(total_ref)

    def analyse(t):
        forced = adjoint[...] + field_ref[t]
        adjoint[...] = forced
        for k in range(levels):
            upper, lower = halves(forced[k * lat_rows : (k + 1) * lat_rows])
            coeffs = (
                dot(fhigh_ref[...], upper, NT) + dot(flow_ref[...], upper, NT) + dot(fhigh_ref[...], lower, NT)
            )
            for p in range(2):
                part = coeffs[p * waves : (p + 1) * waves]
                rounded = part.astype(BF16).astype(F32)
                packed[pl.ds(2 * k + p, waves, stride=group), :] = rounded
                packed[pl.ds(half + 2 * k + p, waves, stride=group), :] = part - rounded

    def spectral_of(m):
        left = packed[pl.ds(pl.multiple_of(m * group, group), group), :].astype(BF16)
        value = pair_sum(dot(left, high[m], NT) + dot(left, low[m], NT))
        total_ref[m] += value
        return value

    def step(s, carry):
        t = times - 1 - s
        analyse(t)
        damp = damp_ref[t]

        def wave(m, inner):
            filtered = spectral_of(m) * damp
            rounded = filtered.astype(BF16).astype(F32)
            left = jnp.where(in_high, rounded, filtered - rounded).astype(BF16)
            back = pair_sum(dot(left, high[m], NN) + dot(left, low[m], NN))
            packed[pl.ds(pl.multiple_of(m * group, group), group), :] = back
            return inner

        lax.fori_loop(0, waves, wave, 0, unroll=8)
        for k in range(levels):
            synth = jnp.concatenate(
                [packed[pl.ds(2 * k + p, waves, stride=group), :] for p in range(2)], 0
            ).T
            upper, lower = halves(synth)
            gridded = dot(upper, fhigh_ref[...], NN) + dot(lower, fhigh_ref[...], NN) + dot(upper, flow_ref[...], NN)
            place = pl.ds(k * lat_rows, lat_rows)
            adjoint[place, :] = tangent_ref[t, place, :] * adjoint[place, :] + gridded
        return carry

    lax.fori_loop(0, times - 1, step, 0)
    analyse(0)

    def last(m, inner):
        spectral_of(m)
        return inner

    lax.fori_loop(0, waves, last, 0, unroll=8)


def sweep(fields, tangent, damp, lat_rows, waves):
    times, rows, lon_cols = fields.shape
    group = damp.shape[1]
    fourier = fourier_rows(lon_cols, waves)
    fhigh = fourier.astype(jnp.bfloat16)
    flow = (fourier - fhigh.astype(np.float32)).astype(jnp.bfloat16)
    mu, diagonal, up, both = legendre_coefficients(lat_rows, waves)
    return pl.pallas_call(
        sweep_kernel,
        in_specs=[pl.BlockSpec(memory_space=pltpu.VMEM)] * 9,
        out_specs=pl.BlockSpec(memory_space=pltpu.VMEM),
        out_shape=jax.ShapeDtypeStruct((waves, group, waves), F32),
        scratch_shapes=[
            pltpu.VMEM((waves * waves, lat_rows), F32),
            pltpu.VMEM((waves, waves, lat_rows), BF16),
            pltpu.VMEM((waves, waves, lat_rows), BF16),
            pltpu.VMEM((waves * group, lat_rows), F32),
            pltpu.VMEM((rows, lon_cols), F32),
        ],
        compiler_params=pltpu.CompilerParams(vmem_limit_bytes=VMEM_BYTES),
    )(fields, tangent, damp, fhigh, flow, mu, diagonal, up, both)


def shards(obs_cell, innovation, tangent, damping, spread, vertical):
    sections = lax.axis_size("tm")
    groups = lax.axis_size("lev")
    me_tm = lax.axis_index("tm")
    me_lev = lax.axis_index("lev")
    lev_dev, lat_rows, lon_cols = tangent.shape[1:]
    levels, waves = damping.shape[1:]
    mine = -(-lev_dev // sections)
    mine += mine % 2
    padded = mine * sections

    def pad_levels(value, axis):
        widths = [(0, 0)] * value.ndim
        widths[axis] = (0, padded - value.shape[axis])
        return jnp.pad(value, widths) if padded > value.shape[axis] else value

    innov = lax.all_to_all(
        pad_levels(innovation[0], 0).reshape(sections, mine, -1), "tm", split_axis=0, concat_axis=0, tiled=True
    )
    cells = lax.all_gather(obs_cell, "tm", axis=0, tiled=True)
    damp_every = lax.all_gather(damping, "tm", axis=0, tiled=True)
    rates = lax.all_to_all(
        pad_levels(tangent[0], 0).reshape(sections, mine * lat_rows, lon_cols),
        "tm", split_axis=0, concat_axis=0, tiled=True,
    )
    fields = forcing_fields(cells, innov, lat_rows, lon_cols)
    damp_block = pad_levels(lax.dynamic_slice_in_dim(damp_every, me_lev * lev_dev, lev_dev, 1), 1)
    damp_mine = lax.dynamic_slice_in_dim(damp_block, me_tm * mine, mine, 1)
    damp_rows = jnp.tile(jnp.repeat(damp_mine, 2, axis=1), (1, 2, 1))
    total = sweep(fields, rates, damp_rows, lat_rows, waves)

    block_m = waves // groups
    block_n = waves // sections
    outgoing = total[:, : 2 * mine].reshape(groups, block_m, mine, 2, sections, block_n)
    outgoing = outgoing.transpose(0, 4, 2, 1, 3, 5).reshape(groups * sections, mine, block_m * 2 * block_n)
    arrived = lax.all_to_all(outgoing, ("lev", "tm"), split_axis=0, concat_axis=0, tiled=True)
    arrived = arrived.reshape(groups, padded, block_m * 2, block_n)[:, :lev_dev]
    arrived = arrived.reshape(levels, block_m * 2, block_n)
    spread_cols = lax.dynamic_slice_in_dim(spread, me_tm * block_n, block_n, 1)
    scaled = (arrived * spread_cols[:, None, :]).reshape(levels, block_m * 2 * block_n)
    result = jnp.einsum("kj,kx->jx", vertical, scaled, precision=PRECISE)
    return result.reshape(levels, block_m, 2, block_n)


def solution(mesh):
    placed = (
        P("tm", None),
        P("tm", "lev", None),
        P("tm", "lev", None, None),
        P("tm", None, None),
        P(),
        P(),
    )
    return jax.shard_map(
        shards, mesh=mesh, in_specs=placed, out_specs=P(None, "lev", None, "tm"), check_vma=False
    )
```

```python
import functools
import math

import jax
import jax.numpy as jnp
import numpy as np
from jax import lax
from jax.experimental import pallas as pl
from jax.experimental.pallas import tpu as pltpu
from jax.sharding import PartitionSpec as P

PRECISE = lax.Precision.HIGHEST
BF16 = jnp.bfloat16
F32 = jnp.float32
NT = (((1,), (1,)), ((), ()))
NN = (((1,), (0,)), ((), ()))
VMEM_BYTES = 62 * 1024 * 1024


def dot(left, right, dims):
    return lax.dot_general(left, right, dims, preferred_element_type=F32)


def halves(value):
    high = value.astype(BF16)
    return high, (value - high.astype(F32)).astype(BF16)


def fourier_rows(lon_count, wave_count):
    index = np.arange(wave_count)[:, None] * np.arange(lon_count)[None, :] % lon_count
    angles = 2.0 * np.pi * index / lon_count
    return (np.concatenate([np.cos(angles), np.sin(angles)], 0) * np.sqrt(2.0 / lon_count)).astype(np.float32)


def legendre_coefficients(lat_count, wave_count):
    phi = (np.arange(lat_count) + 0.5) * np.pi / lat_count - 0.5 * np.pi
    orders = np.arange(wave_count).astype(np.float64)
    lead = np.array(
        [
            -0.5 * math.log(2.0)
            + 0.5 * (math.lgamma(m + 1.5) - math.lgamma(1.5) - math.lgamma(m + 1.0))
            for m in range(wave_count)
        ]
    )
    weight = np.sqrt(np.pi * np.cos(phi) / lat_count)
    diagonal = weight[:, None] * np.exp(lead[None, :] + orders[None, :] * np.log(np.cos(phi))[:, None])
    mu = np.broadcast_to(np.sin(phi)[:, None], (lat_count, wave_count))
    degree = orders[:, None]
    above = degree > orders[None, :]
    gap = np.where(above, degree**2 - orders[None, :] ** 2, 1.0)
    up = np.where(above, np.sqrt(np.maximum(4.0 * degree**2 - 1.0, 0.0) / gap), 0.0)
    lower = degree - 1.0
    down = np.sqrt(np.maximum(lower**2 - orders[None, :] ** 2, 0.0) / np.maximum(4.0 * lower**2 - 1.0, 1.0))
    both = up * down
    return [np.asarray(a, np.float32) for a in (mu, diagonal, up, both)]


def forcing_kernel(lat_rows, lon_cols, cell_ref, innov_ref, out_ref):
    cells = cell_ref[0]
    width = cells.shape[1]
    rows = cells // lon_cols
    cols = cells - rows * lon_cols
    innov = innov_ref[0]
    levels = innov.shape[0]
    hit = lax.broadcasted_iota(jnp.int32, (lat_rows, width), 0) == rows
    spread_cols = jnp.where(
        lax.broadcasted_iota(jnp.int32, (lon_cols, width), 0) == cols, 1.0, 0.0
    ).astype(BF16)
    high = innov.astype(BF16).astype(F32)
    low = innov - high
    pieces = [jnp.where(hit, part[k : k + 1, :], 0.0).astype(BF16) for part in (high, low) for k in range(levels)]
    field = dot(jnp.concatenate(pieces, 0), spread_cols, NT)
    field = field[: levels * lat_rows] + field[levels * lat_rows :]

    @pl.when(pl.program_id(1) == 0)
    def _():
        out_ref[0] = field

    @pl.when(pl.program_id(1) > 0)
    def _():
        out_ref[0] += field


def forcing_fields(cells, innov, lat_rows, lon_cols):
    times, levels, count = innov.shape
    width = math.gcd(count, 2048)
    body = functools.partial(forcing_kernel, lat_rows, lon_cols)
    return pl.pallas_call(
        body,
        grid=(times, count // width),
        in_specs=[
            pl.BlockSpec((1, 1, width), lambda t, c: (t, 0, c)),
            pl.BlockSpec((1, levels, width), lambda t, c: (t, 0, c)),
        ],
        out_specs=pl.BlockSpec((1, levels * lat_rows, lon_cols), lambda t, c: (t, 0, 0)),
        out_shape=jax.ShapeDtypeStruct((times, levels * lat_rows, lon_cols), F32),
        compiler_params=pltpu.CompilerParams(vmem_limit_bytes=VMEM_BYTES),
        cost_estimate=pl.CostEstimate(
            flops=4 * times * levels * lat_rows * lon_cols * count, bytes_accessed=8 * 2**20, transcendentals=0
        ),
    )(cells.reshape(times, 1, count), innov)


def sweep_kernel(
    field_ref, tangent_ref, damp_ref, fhigh_ref, flow_ref, mu_ref, diag_ref, up_ref, both_ref,
    total_ref, table, high, low, packed, adjoint,
):
    times, rows, lon_cols = field_ref.shape
    lat_rows, waves = mu_ref.shape
    levels = rows // lat_rows
    group = damp_ref.shape[1]
    half = group // 2

    orders = lax.broadcasted_iota(jnp.int32, (lat_rows, waves), 1)

    def advance(n, state):
        one, two = state
        recurred = up_ref[pl.ds(n, 1), :] * (mu_ref[...] * one) - both_ref[pl.ds(n, 1), :] * two
        value = jnp.where(orders == n, diag_ref[...], recurred)
        table[pl.ds(n, waves, stride=waves), :] = value.T
        return value, one

    zero = 0.0 * mu_ref[...]
    lax.fori_loop(0, waves, advance, (zero, zero), unroll=8)

    def split(m, carry):
        upper, lower = halves(table[pl.ds(m * waves, waves), :])
        high[m] = upper
        low[m] = lower
        return carry

    lax.fori_loop(0, waves, split, 0, unroll=4)

    def pair_sum(value):
        return value + pltpu.roll(value, half, 0)

    in_high = lax.broadcasted_iota(jnp.int32, (group, waves), 0) < half
    adjoint[...] = jnp.zeros_like(adjoint)
    total_ref[...] = jnp.zeros_like(total_ref)

    def analyse(t):
        forced = adjoint[...] + field_ref[t]
        adjoint[...] = forced
        for k in range(levels):
            upper, lower = halves(forced[k * lat_rows : (k + 1) * lat_rows])
            coeffs = (
                dot(fhigh_ref[...], upper, NT) + dot(flow_ref[...], upper, NT) + dot(fhigh_ref[...], lower, NT)
            )
            for p in range(2):
                part = coeffs[p * waves : (p + 1) * waves]
                rounded = part.astype(BF16).astype(F32)
                packed[pl.ds(2 * k + p, waves, stride=group), :] = rounded
                packed[pl.ds(half + 2 * k + p, waves, stride=group), :] = part - rounded

    batch = math.gcd(waves, 16)

    def lanes_of(b):
        return pl.ds(pl.multiple_of(b * batch * group, batch * group), batch * group)

    def parts_of(value):
        return [value[u * group : (u + 1) * group] for u in range(batch)]

    def product(lefts, b, dims):
        return [
            pair_sum(dot(left, high[b * batch + u], dims) + dot(left, low[b * batch + u], dims))
            for u, left in enumerate(lefts)
        ]

    def spectral_of(b):
        lefts = parts_of(packed[lanes_of(b), :].astype(BF16))
        values = product(lefts, b, NT)
        total_ref[lanes_of(b), :] += jnp.concatenate(values, 0)
        return values

    def step(s, carry):
        t = times - 1 - s
        analyse(t)
        damp = damp_ref[t]

        def wave(b, inner):
            lefts = []
            for value in spectral_of(b):
                filtered = value * damp
                rounded = filtered.astype(BF16).astype(F32)
                lefts.append(jnp.where(in_high, rounded, filtered - rounded).astype(BF16))
            packed[lanes_of(b), :] = jnp.concatenate(product(lefts, b, NN), 0)
            return inner

        lax.fori_loop(0, waves // batch, wave, 0)
        for k in range(levels):
            synth = jnp.concatenate(
                [packed[pl.ds(2 * k + p, waves, stride=group), :] for p in range(2)], 0
            ).T
            upper, lower = halves(synth)
            gridded = dot(upper, fhigh_ref[...], NN) + dot(lower, fhigh_ref[...], NN) + dot(upper, flow_ref[...], NN)
            place = pl.ds(k * lat_rows, lat_rows)
            adjoint[place, :] = tangent_ref[t, place, :] * adjoint[place, :] + gridded
        return carry

    lax.fori_loop(0, times - 1, step, 0)
    analyse(0)

    def last(b, inner):
        spectral_of(b)
        return inner

    lax.fori_loop(0, waves // batch, last, 0)


def sweep(fields, tangent, damp, lat_rows, waves):
    times, rows, lon_cols = fields.shape
    group = damp.shape[1]
    fourier = fourier_rows(lon_cols, waves)
    fhigh = fourier.astype(jnp.bfloat16)
    flow = (fourier - fhigh.astype(np.float32)).astype(jnp.bfloat16)
    mu, diagonal, up, both = legendre_coefficients(lat_rows, waves)
    return pl.pallas_call(
        sweep_kernel,
        in_specs=[pl.BlockSpec(memory_space=pltpu.VMEM)] * 9,
        out_specs=pl.BlockSpec(memory_space=pltpu.VMEM),
        out_shape=jax.ShapeDtypeStruct((waves * group, waves), F32),
        scratch_shapes=[
            pltpu.VMEM((waves * waves, lat_rows), F32),
            pltpu.VMEM((waves, waves, lat_rows), BF16),
            pltpu.VMEM((waves, waves, lat_rows), BF16),
            pltpu.VMEM((waves * group, lat_rows), F32),
            pltpu.VMEM((rows, lon_cols), F32),
        ],
        compiler_params=pltpu.CompilerParams(vmem_limit_bytes=VMEM_BYTES),
    )(fields, tangent, damp, fhigh, flow, mu, diagonal, up, both)


def shards(obs_cell, innovation, tangent, damping, spread, vertical):
    sections = lax.axis_size("tm")
    groups = lax.axis_size("lev")
    me_tm = lax.axis_index("tm")
    me_lev = lax.axis_index("lev")
    lev_dev, lat_rows, lon_cols = tangent.shape[1:]
    levels, waves = damping.shape[1:]
    mine = -(-lev_dev // sections)
    mine += mine % 2
    padded = mine * sections

    def pad_levels(value, axis):
        widths = [(0, 0)] * value.ndim
        widths[axis] = (0, padded - value.shape[axis])
        return jnp.pad(value, widths) if padded > value.shape[axis] else value

    count = obs_cell.shape[1]
    damp_block = pad_levels(lax.dynamic_slice_in_dim(damping[0], me_lev * lev_dev, lev_dev, 0), 0)
    damp_block = damp_block.reshape(sections, mine * waves)
    damp_deep = -(-mine * waves // count)
    damp_block = jnp.pad(damp_block, ((0, 0), (0, damp_deep * count - mine * waves)))
    message = jnp.concatenate(
        [
            pad_levels(innovation[0], 0).reshape(sections, mine, count),
            jnp.broadcast_to(obs_cell.astype(F32)[None], (sections, 1, count)),
            damp_block.reshape(sections, damp_deep, count),
        ],
        1,
    )
    message = lax.all_to_all(message, "tm", split_axis=0, concat_axis=0, tiled=True)
    innov = message[:, :mine]
    cells = message[:, mine].astype(jnp.int32)
    damp_mine = message[:, mine + 1 :].reshape(sections, damp_deep * count)[:, : mine * waves]
    damp_mine = damp_mine.reshape(sections, mine, waves)
    rates = lax.all_to_all(
        pad_levels(tangent[0], 0).reshape(sections, mine * lat_rows, lon_cols),
        "tm", split_axis=0, concat_axis=0, tiled=True,
    )
    fields = forcing_fields(cells, innov, lat_rows, lon_cols)
    damp_rows = jnp.tile(jnp.repeat(damp_mine, 2, axis=1), (1, 2, 1))
    total = sweep(fields, rates, damp_rows, lat_rows, waves)

    block_m = waves // groups
    block_n = waves // sections
    outgoing = total.reshape(waves, 4 * mine, waves)[:, : 2 * mine].reshape(groups, block_m, mine, 2, sections, block_n)
    outgoing = outgoing.transpose(0, 4, 2, 1, 3, 5).reshape(groups * sections, mine, block_m * 2 * block_n)
    arrived = lax.all_to_all(outgoing, ("lev", "tm"), split_axis=0, concat_axis=0, tiled=True)
    arrived = arrived.reshape(groups, padded, block_m * 2, block_n)[:, :lev_dev]
    arrived = arrived.reshape(levels, block_m * 2, block_n)
    spread_cols = lax.dynamic_slice_in_dim(spread, me_tm * block_n, block_n, 1)
    scaled = (arrived * spread_cols[:, None, :]).reshape(levels, block_m * 2 * block_n)
    result = jnp.einsum("kj,kx->jx", vertical, scaled, precision=PRECISE)
    return result.reshape(levels, block_m, 2, block_n)


def solution(mesh):
    placed = (
        P("tm", None),
        P("tm", "lev", None),
        P("tm", "lev", None, None),
        P("tm", None, None),
        P(),
        P(),
    )
    return jax.shard_map(
        shards, mesh=mesh, in_specs=placed, out_specs=P(None, "lev", None, "tm"), check_vma=False
    )
```
